512 devices in a mesh: slab: 128 (over y, z, core), walk: 4 (over x).
Axes of the slice: x: 4, y: 8, z: 8, core: 2. Of those that a mesh axis runs over, the one named last changes fastest.
Arguments:
- bias_grid: float32 [512, 512, 512], P('slab', 'walk'), may hold values from 0 to 12, as said below
- hill_slab: int32 [1024, 64, 1], P(('slab', 'walk')), may hold values from 0 to 127; in each aligned block of 128 rows (0 to 127, 128 to 255, ..., all dimensions but the last counted through in order) at most 4 rows name the same one
- hill_row: int32 [1024, 64], P(('slab', 'walk')), may hold values from 0 to 3
- hill_col: int32 [1024, 64], P(('slab', 'walk')), may hold values from 0 to 511
- hill_depth: int32 [1024, 64], P(('slab', 'walk')), may hold values from 0 to 511
- hill_level: int32 [1024, 64], P(('slab', 'walk')), may hold values from 0 to 7
- hill_count: int32 [1024], P(('slab', 'walk')), may hold values from 1 to 64
- height_levels: float32 [8], replicated, may hold values from 0.5 to 2
Outputs:
- new_bias: float32 [512, 512, 512], P('slab', 'walk')
- free_energy: float32 [512, 512, 512], P('slab', 'walk')
The draws below stay inside these ranges and needn't reach their ends.
Inputs may be any that keep to these rules, and one draw needn't show every extreme that they name: `bias_grid`: the bias is not negative. `hill_slab`: among the hills of one device's walkers (128 hills in a row of the flattened walkers and hills), no slab is named more than 4 times, and in some such blocks one slab is named exactly 4 times.
All inputs are finite; a program needn't handle non-finite values.
Results may differ from the reference program's by a relative error of at most 0.000082.
Values sent between devices are 32-bit elements; how exact they have to be, the bound alone decides.
No kernel may reach another device: no remote copies, remote signals or barrier semaphores. Data moves between devices by JAX's collectives and lax.ppermute only.
A program may use at most 64 MiB of HBM per device.

```python
import math
import jax
import jax.numpy as jnp
import numpy as np
from jax import lax

ROWS_DEV = 4
DEPTH = 512
HILLS = 64
WALKERS_DEV = 2
LEVELS = 8
REACH = 8
CAP = 4
GRID_ROWS = 512
GRID_COLS = 512
WALKERS = 1024
N_SLAB = 128


def draw_bias_grid(key, part):
    rough_key = jax.random.fold_in(key, 11)
    row_key = jax.random.fold_in(key, 12)
    col_key = jax.random.fold_in(key, 13)
    depth_key = jax.random.fold_in(key, 14)
    rough_cells = jax.random.uniform(rough_key, (GRID_ROWS, GRID_COLS, DEPTH), jnp.float32)
    row_scale = jnp.exp(jax.random.uniform(row_key, (GRID_ROWS, 1, 1), jnp.float32, math.log(0.5), math.log(4.0)))
    col_scale = jnp.exp(jax.random.uniform(col_key, (1, GRID_COLS, 1), jnp.float32, math.log(0.8), math.log(2.0)))
    depth_scale = jnp.exp(jax.random.uniform(depth_key, (1, 1, DEPTH), jnp.float32, math.log(0.8), math.log(1.25)))
    rough_part = rough_cells * row_scale * col_scale * depth_scale
    return rough_part


def with_ends(values, stream_key, low, top_value):
    longest = values.shape.index(max(values.shape))
    spots = []
    for shift in (0, 1):
        where = [jax.random.randint(jax.random.fold_in(stream_key, axis), (), 0, length) for axis, length in enumerate(values.shape)]
        where[longest] = (where[longest] + shift) % values.shape[longest]
        spots.append(tuple(where))
    return values.at[spots[0]].set(low).at[spots[1]].set(top_value)


def shared_out(own_key, own, number, rows, number_of, top, bound, slope):
    sequence = jax.random.permutation(own_key, number_of)
    heavy_load, usual = shares(number_of, rows * top, bound, slope, True), shares(number_of, rows * top, bound, slope, False)
    places = jnp.arange(number_of)

    def named(sizes, offset_by):
        used = int((sizes > 0).sum())
        fixed = max(1, used // 4)
        moved = fixed + (places - fixed + offset_by * (used - fixed)) % max(1, number_of - fixed)
        return jnp.zeros((number_of,), jnp.int32).at[sequence[jnp.where(places < fixed, places, moved)]].set(jnp.asarray(sizes, jnp.int32))

    sizes = jnp.where(number % 4 == 0, named(heavy_load, number // 4), named(usual, number - number // 4 - 1))
    mixed = jax.random.permutation(jax.random.fold_in(own, 3), number_of)
    source_of, taker = mixed[0:number_of // 2 * 2:2], mixed[1:number_of // 2 * 2:2]
    slack = jnp.minimum(sizes[source_of] - 1, bound - sizes[taker]) // 2
    slack = jnp.where((source_of == sequence[0]) | (taker == sequence[0]) | (sizes[taker] == 0), 0, jnp.maximum(slack, 0))
    moved = jax.random.randint(jax.random.fold_in(own, 4), (number_of // 2,), 0, 1 << 20) % (slack + 1)
    sizes = sizes.at[source_of].add(-moved).at[taker].add(moved)
    members = jnp.searchsorted(jnp.cumsum(sizes), jnp.arange(rows * top), side="right").astype(jnp.int32)
    table = members.reshape(top, rows).T
    table = table[jax.random.permutation(jax.random.fold_in(own, 1), rows)]
    offset_by = jax.random.randint(jax.random.fold_in(own, 2), (rows, 1), 0, top)
    return jnp.take_along_axis(table, (jnp.arange(top)[None, :] + offset_by) % top, axis=1)


def shares(count, total, bound, skew, full):
    portions = [(1 << 20) // math.isqrt(rank ** skew) + 1 for rank in range(1, count + 1)]
    largest = bound if full else min(bound, max(-(-total // count), total * portions[0] // sum(portions)))
    least = 1 if total - largest >= count - 1 else 0
    counts, surplus = [largest] + [least] * (count - 1), total - largest - least * (count - 1)
    while surplus > 0:
        free = [i for i in range(1, count) if counts[i] < largest] or [i for i in range(1, count) if counts[i] < bound]
        whole, budget = sum([portions[i] for i in free]), surplus
        for i in free:
            extra = min(bound - counts[i], max(1, budget * portions[i] // whole), surplus)
            counts[i] = counts[i] + extra
            surplus = surplus - extra
    return np.array(counts)


def setup_inputs(seed: int = 0) -> dict:
    streams_of = jax.random.split(jax.random.key(seed), 9)
    bias_grid = draw_bias_grid(jax.random.fold_in(streams_of[8], 71), 0)
    hill_slab_keys = jax.random.split(jax.random.fold_in(streams_of[1], 1), WALKERS * HILLS // (WALKERS_DEV * HILLS))
    hill_slab_turns = jax.random.permutation(jax.random.fold_in(streams_of[1], 3), WALKERS * HILLS // (WALKERS_DEV * HILLS))
    hill_slab = jax.vmap(lambda own, number: shared_out(jax.random.fold_in(streams_of[1], 2), own, number, WALKERS_DEV * HILLS, N_SLAB, 1, CAP, 2))(hill_slab_keys, hill_slab_turns).reshape((WALKERS, HILLS, 1))
    hill_row = with_ends(jax.random.randint(streams_of[2], (WALKERS, HILLS), 0, ROWS_DEV), jax.random.fold_in(streams_of[2], 1), 0, ROWS_DEV - 1).astype(jnp.int32)
    hill_col = with_ends(jax.random.randint(streams_of[3], (WALKERS, HILLS), 0, GRID_COLS), jax.random.fold_in(streams_of[3], 1), 0, GRID_COLS - 1).astype(jnp.int32)
    hill_depth = with_ends(jax.random.randint(streams_of[4], (WALKERS, HILLS), 0, DEPTH), jax.random.fold_in(streams_of[4], 1), 0, DEPTH - 1).astype(jnp.int32)
    hill_level = with_ends(jax.random.randint(streams_of[5], (WALKERS, HILLS), 0, LEVELS), jax.random.fold_in(streams_of[5], 1), 0, LEVELS - 1).astype(jnp.int32)
    hill_count = with_ends(jax.random.randint(streams_of[6], (WALKERS,), 1, HILLS + 1), jax.random.fold_in(streams_of[6], 1), 1, HILLS).astype(jnp.int32)
    height_levels = jnp.clip(jnp.exp(jax.random.uniform(streams_of[7], (LEVELS,), jnp.float32, math.log(0.5), math.log(2.0))), 0.5, 2.0)
    return dict(bias_grid=bias_grid, hill_slab=hill_slab, hill_row=hill_row, hill_col=hill_col, hill_depth=hill_depth, hill_level=hill_level, hill_count=hill_count, height_levels=height_levels)


BASE_HEIGHT = 1.2
TEMPER = 4.0
SIGMA_SHARE = 0.3125
FREE_SCALE = 10.0 / 9.0


def fold_axis(padded, radius, extent, axis):
    inner = lax.slice_in_dim(padded, radius, radius + extent, axis=axis)
    low_part = lax.slice_in_dim(padded, 0, radius, axis=axis)
    high_part = lax.slice_in_dim(padded, radius + extent, 2 * radius + extent, axis=axis)
    head = lax.slice_in_dim(inner, 0, radius, axis=axis) + high_part
    middle = lax.slice_in_dim(inner, radius, extent - radius, axis=axis)
    tail = lax.slice_in_dim(inner, extent - radius, extent, axis=axis) + low_part
    return jnp.concatenate([head, middle, tail], axis=axis)


def reference(bias_grid, hill_slab, hill_row, hill_col, hill_depth, hill_level, hill_count, height_levels):
    grid_rows, grid_cols, grid_depth = bias_grid.shape
    radius = REACH
    centre_row = (hill_slab[:, :, 0] * ROWS_DEV + hill_row).reshape(-1).astype(jnp.int32)
    centre_col = hill_col.reshape(-1).astype(jnp.int32)
    centre_depth = hill_depth.reshape(-1).astype(jnp.int32)
    is_live = (jnp.arange(HILLS, dtype=jnp.int32)[None, :] < hill_count[:, None]).reshape(-1)
    level_match = hill_level.reshape(-1)[:, None] == jnp.arange(LEVELS, dtype=jnp.int32)[None, :]
    base_height = jnp.sum(jnp.where(level_match, height_levels[None, :], 0.0), axis=1)
    base_height = jnp.where(is_live, BASE_HEIGHT * base_height, 0.0)
    height = base_height * jnp.exp(-bias_grid[centre_row, centre_col, centre_depth] / TEMPER)
    spread = SIGMA_SHARE * radius
    distance = (jnp.arange(2 * radius, dtype=jnp.int32) - radius).astype(jnp.float32)
    profile = jnp.exp(-(distance * distance) / (2.0 * spread * spread))

    def add_hill(padded, hill):
        weight, row_at, col_at, depth_at = hill
        patch = (weight * profile)[:, None, None] * profile[None, :, None] * profile[None, None, :]
        current = lax.dynamic_slice(padded, (row_at, col_at, depth_at), (2 * radius, 2 * radius, 2 * radius))
        return lax.dynamic_update_slice(padded, current + patch, (row_at, col_at, depth_at)), None

    start = jnp.zeros((grid_rows + 2 * radius, grid_cols + 2 * radius, grid_depth + 2 * radius), jnp.float32)
    padded, unused = lax.scan(add_hill, start, (height, centre_row, centre_col, centre_depth))
    folded = fold_axis(padded, radius, grid_rows, 0)
    folded = fold_axis(folded, radius, grid_cols, 1)
    deposit = fold_axis(folded, radius, grid_depth, 2)
    new_bias = bias_grid + deposit
    highest = jnp.max(new_bias)
    free_energy = FREE_SCALE * (highest - new_bias)
    return new_bias, free_energy
```

```python
import functools

import jax
import jax.numpy as jnp
from jax import lax
from jax.experimental import pallas as pl
from jax.experimental.pallas import tpu as pltpu
from jax.sharding import Mesh
from jax.sharding import PartitionSpec as P

SLAB = ("y", "z", "c")
CHIP_ROW = ("c", "walk")
EVERY = SLAB + ("walk",)

BASE_HEIGHT = 1.2
TEMPER = 4.0
SIGMA_SHARE = 0.3125
FREE_SCALE = 10.0 / 9.0

LANES = 128
SLOTS = 4
NEAR = 5
FIELD = 32
UNIT = 32

F32 = jnp.float32
BF16 = jnp.bfloat16
I32 = jnp.int32


def iota(shape, dim, dtype=I32):
    return lax.broadcasted_iota(dtype, shape, dim)


def parts_of(x, count):
    parts = []
    for i in range(count):
        part = x.astype(BF16)
        parts.append(part)
        if i + 1 < count:
            x = x - part.astype(F32)
    return parts


def dot_t(a, b):
    return lax.dot_general(a, b, (((1,), (1,)), ((), ())), preferred_element_type=F32)


def dot(a, b):
    return jnp.dot(a, b, preferred_element_type=F32)


def pack_kernel(rows_dev, count, levels, slab, row, col, depth, level, out):
    walkers, hills = slab.shape
    n_slab = out.shape[1]

    def flat(ref):
        return jnp.concatenate([ref[w : w + 1, :] for w in range(walkers)], axis=1)

    total = walkers * hills
    index = iota((1, total), 1)
    limit = jnp.full((1, total), count[0], I32)
    for w in range(1, walkers):
        limit = jnp.where(index < w * hills, limit, count[w] + w * hills)
    live = index < limit
    target = flat(slab)
    lev = flat(level)
    base = jnp.zeros((1, total), F32)
    for i in range(levels.shape[0]):
        base = jnp.where(lev == i, levels[i], base)
    base = jnp.where(live, BASE_HEIGHT * base, 0.0)
    fields = [
        base,
        (target * rows_dev + flat(row)).astype(F32),
        flat(col).astype(F32),
        flat(depth).astype(F32),
    ]
    match = iota((n_slab, total), 0) == target
    earlier = (iota((total, total), 0) < iota((total, total), 1)).astype(F32).astype(BF16)
    rank = dot(match.astype(F32).astype(BF16), earlier)
    rank = jnp.where(match, rank, -1.0)
    place = iota((LANES, total), 0)
    masks, values = [], []
    for slot in range(SLOTS):
        masks.append((rank == slot).astype(F32).astype(BF16))
        value = jnp.zeros((LANES, total), F32)
        for f, field in enumerate(fields):
            value = jnp.where(place == f * FIELD + slot, field, value)
        values.append(value)
    mask = jnp.concatenate(masks, axis=1)
    own = jnp.zeros((n_slab, LANES), F32)
    for part in parts_of(jnp.concatenate(values, axis=1), 3):
        own = own + dot_t(mask, part)
    message = jnp.zeros((n_slab, LANES), F32)
    for k in range(NEAR):
        part = pltpu.roll(own, (NEAR // 2 - k) % n_slab, 0)
        message = message + (pltpu.roll(part, k * SLOTS, 1) if k else part)
    for w in range(out.shape[0]):
        out[w] = message


def positions(active, chain, block):
    earlier = (iota((LANES, LANES), 0) < iota((LANES, LANES), 1)).astype(F32).astype(BF16)
    ones = jnp.ones((LANES, LANES), F32).astype(BF16)
    found, most = [], None
    for j in range(block):
        a = active[:, j * LANES : (j + 1) * LANES]
        ab = a.astype(BF16)
        total = dot(ab, ones)
        ahead = dot(chain, total.astype(BF16))
        found.append(jnp.where(a > 0.0, dot(ab, earlier) + ahead, -1.0))
        count = ahead + total
        most = count if most is None else jnp.maximum(most, count)
    return found, jnp.max(most).astype(I32)


def chain_of(rows):
    i, j = iota((rows, rows), 0), iota((rows, rows), 1)
    same = lax.shift_right_logical(i, 2) == lax.shift_right_logical(j, 2)
    return (same & (j < i)).astype(F32).astype(BF16)


def height_kernel(rows_dev, cols_dev, grid_cols, recv, bias, out, table, hi, mid, lo, found):
    senders = recv.shape[0]
    blocks = senders // LANES
    cells, depth_bins = bias.shape
    walk = lax.axis_index("walk")
    for j in range(blocks):
        table[:, j * LANES : (j + 1) * LANES] = recv[j * LANES : (j + 1) * LANES, :].T
    first = (NEAR // 2) * SLOTS
    base = table[first : first + 8, :]
    row = table[FIELD + first : FIELD + first + 8, :].astype(I32)
    col = table[2 * FIELD + first : 2 * FIELD + first + 8, :].astype(I32)
    depth = table[3 * FIELD + first : 3 * FIELD + first + 8, :]
    col = col - walk * cols_dev
    held = (iota(base.shape, 0) < SLOTS) & (base != 0.0) & (col >= 0) & (col < cols_dev)
    cell = ((row & (rows_dev - 1)) * cols_dev + col).astype(F32)
    place, most = positions(held.astype(F32), chain_of(8), blocks)
    bias_parts = parts_of(bias[...], 3)
    hi[...], mid[...], lo[...] = bias_parts
    found[...] = jnp.zeros_like(found)

    def one_pass(t, carry):
        number = (iota((UNIT, LANES), 0) + t * UNIT).astype(F32)
        cells_at, depths_at, hits = [], [], []
        for j in range(blocks):
            at = slice(j * LANES, (j + 1) * LANES)
            c = jnp.zeros((UNIT, LANES), F32)
            d = jnp.zeros((UNIT, LANES), F32)
            for slot in range(SLOTS):
                hit = place[j][slot : slot + 1, :] == number
                hits.append(hit)
                c = jnp.where(hit, cell[slot : slot + 1, at], c)
                d = jnp.where(hit, depth[slot : slot + 1, at], d)
            cells_at.append(jnp.sum(c, axis=1, keepdims=True))
            depths_at.append(jnp.sum(d, axis=1, keepdims=True))
        cells_at = jnp.concatenate(cells_at, axis=0).astype(I32)
        depths_at = jnp.concatenate(depths_at, axis=0).astype(I32)
        count = blocks * UNIT
        pick = (iota((count, cells), 1) == cells_at).astype(F32).astype(BF16)
        lines = dot(pick, hi[...]) + dot(pick, mid[...]) + dot(pick, lo[...])
        value = jnp.sum(
            jnp.where(iota((count, depth_bins), 1) == depths_at, lines, 0.0),
            axis=1,
            keepdims=True,
        )
        for j in range(blocks):
            v = value[j * UNIT : (j + 1) * UNIT, :]
            for slot in range(SLOTS):
                back = jnp.sum(
                    jnp.where(hits[j * SLOTS + slot], v, 0.0), axis=0, keepdims=True
                )
                found[slot : slot + 1, j * LANES : (j + 1) * LANES] += back
        return carry

    lax.fori_loop(0, lax.div(most + (UNIT - 1), UNIT), one_pass, 0)
    height = jnp.where(held, base * jnp.exp(-found[...] / TEMPER), 0.0)
    for i in range(out.shape[0]):
        out[i] = height[:SLOTS, :]


def profile(offset, radius, extent):
    spread = SIGMA_SHARE * radius
    shifted = (offset + radius) & (extent - 1)
    t = (shifted - radius).astype(F32)
    return jnp.where(shifted < 2 * radius, jnp.exp(-(t * t) / (2.0 * spread * spread)), 0.0)


def deposit_kernel(
    rows_dev, cols_dev, grid_rows, grid_cols, radius,
    table, below, own, above, bias, out, peak, lists, heights, rows_of, row_hi, row_lo, col_hi, col_lo,
):
    senders = table.shape[1]
    blocks = senders // LANES
    cells, depth_bins = bias.shape
    slab = lax.axis_index(SLAB)
    walk = lax.axis_index("walk")
    start = lax.axis_index("c")
    chip = own.shape[0]
    for i in range(chip):
        lists[i] = below[i]
        lists[chip + i] = own[i]
        lists[2 * chip + i] = above[i]
    used = 8 * ((NEAR * SLOTS + 7) // 8)
    heights[...] = jnp.zeros_like(heights)
    for k in range(NEAR):
        heights[k * SLOTS : (k + 1) * SLOTS, :] = lists[start + k]
    base = table[0:used, :]
    row = table[FIELD : FIELD + used, :]
    col = table[2 * FIELD : 2 * FIELD + used, :]
    depth = table[3 * FIELD : 3 * FIELD + used, :]
    reached = ((col.astype(I32) - walk * cols_dev + (radius - 1)) & (grid_cols - 1)) < (
        cols_dev + 2 * radius - 1
    )
    active = (iota(base.shape, 0) < NEAR * SLOTS) & (base != 0.0) & reached
    place, most = positions(active.astype(F32), chain_of(used), blocks)
    count = NEAR * blocks * UNIT
    chunks = count // LANES
    out[...] = bias[...]

    def one_pass(t, carry):
        number = (iota((UNIT, LANES), 0) + t * UNIT).astype(F32)
        lane = iota((UNIT, LANES), 1)
        for k in range(NEAR):
            for j in range(blocks):
                at = slice(j * LANES, (j + 1) * LANES)
                sums = [jnp.zeros((UNIT, LANES), F32) for _ in range(4)]
                for slot in range(SLOTS):
                    i = k * SLOTS + slot
                    hit = place[j][i : i + 1, :] == number
                    for f, field in enumerate((row, col, depth, heights)):
                        sums[f] = jnp.where(hit, field[i : i + 1, at], sums[f])
                cols = [jnp.sum(s, axis=1, keepdims=True) for s in sums]
                packed = jnp.where(
                    lane == 0,
                    cols[0],
                    jnp.where(lane == 1, cols[1], jnp.where(lane == 2, cols[2], cols[3])),
                )
                u = (k * blocks + j) * UNIT
                rows_of[u : u + UNIT, :] = packed
        for h in range(chunks):
            at = slice(h * LANES, (h + 1) * LANES)
            block = rows_of[at, :]
            turned = block.T
            row_at = turned[0:1, :].astype(I32)
            col_at = turned[1:2, :].astype(I32)
            height_at = turned[3:4, :]
            depth_at = block[:, 2:3].astype(I32)
            col_part = profile(
                iota((cols_dev, LANES), 0) + walk * cols_dev - col_at, radius, grid_cols
            )
            for r in range(rows_dev):
                row_part = profile(slab * rows_dev + r - row_at, radius, grid_rows) * height_at
                first, second = parts_of(col_part * row_part, 2)
                row_hi[r * cols_dev : (r + 1) * cols_dev, at] = first
                row_lo[r * cols_dev : (r + 1) * cols_dev, at] = second
            first, second = parts_of(
                profile(iota((LANES, depth_bins), 1) - depth_at, radius, depth_bins), 2
            )
            col_hi[at, :] = first
            col_lo[at, :] = second
        added = dot(row_hi[...], col_lo[...]) + dot(row_lo[...], col_hi[...])
        out[...] += added + dot(row_hi[...], col_hi[...])
        return carry

    lax.fori_loop(0, lax.div(most + (UNIT - 1), UNIT), one_pass, 0)
    peak[...] = jnp.full(peak.shape, jnp.max(out[...]), F32)


def spread_max_kernel(recv, out):
    out[...] = jnp.full(out.shape, jnp.max(recv[...]), F32)


def free_kernel(recv, bias, out):
    out[...] = FREE_SCALE * (jnp.max(recv[...]) - bias[...])


def call(body, name, out_shape, *operands, smem=0, scratch=()):
    in_specs = [
        pl.BlockSpec(memory_space=pltpu.SMEM if i < smem else pltpu.VMEM)
        for i in range(len(operands))
    ]
    out_specs = jax.tree.map(lambda s: pl.BlockSpec(memory_space=pltpu.VMEM), out_shape)
    return pl.pallas_call(
        body,
        name=name,
        out_shape=out_shape,
        in_specs=in_specs,
        out_specs=out_specs,
        scratch_shapes=list(scratch),
    )(*operands)


def shape_of(*dims):
    return jax.ShapeDtypeStruct(dims, F32)


def swap(array, axes):
    return lax.all_to_all(array, axes, 0, 0, tiled=True)


def per_device(
    bias_grid, hill_slab, hill_row, hill_col, hill_depth, hill_level, hill_count, height_levels
):
    rows_dev, cols_dev, depth_bins = bias_grid.shape
    n_slab = lax.axis_size(SLAB)
    n_walk = lax.axis_size("walk")
    radius = 2 * rows_dev
    grid_rows = rows_dev * n_slab
    grid_cols = cols_dev * n_walk
    senders = n_slab * n_walk
    cells = rows_dev * cols_dev
    chip = lax.axis_size("c")
    bias = bias_grid.reshape(cells, depth_bins)

    message = call(
        functools.partial(pack_kernel, rows_dev),
        "pack",
        shape_of(n_walk, n_slab, LANES),
        hill_count,
        height_levels,
        hill_slab[:, :, 0],
        hill_row,
        hill_col,
        hill_depth,
        hill_level,
        smem=2,
    )
    recv = swap(message.reshape(senders, 1, LANES), ("walk",) + SLAB).reshape(senders, LANES)

    own, table = call(
        functools.partial(height_kernel, rows_dev, cols_dev, grid_cols),
        "heights",
        (shape_of(chip * n_walk, SLOTS, senders), shape_of(LANES, senders)),
        recv,
        bias,
        scratch=[pltpu.VMEM((cells, depth_bins), BF16)] * 3 + [pltpu.VMEM((8, senders), F32)],
    )
    own = swap(own, CHIP_ROW).reshape(chip, n_walk, SLOTS, senders).sum(axis=1)
    ring = range(n_slab)
    below = lax.ppermute(own, SLAB, [(s, (s + chip) % n_slab) for s in ring])
    above = lax.ppermute(own, SLAB, [(s, (s - chip) % n_slab) for s in ring])

    hills = NEAR * (senders // LANES) * UNIT
    used = 8 * ((NEAR * SLOTS + 7) // 8)
    new_bias, peak = call(
        functools.partial(deposit_kernel, rows_dev, cols_dev, grid_rows, grid_cols, radius),
        "deposit",
        (shape_of(cells, depth_bins), shape_of(lax.axis_size(("z", "c")), LANES)),
        table,
        below,
        own,
        above,
        bias,
        scratch=[
            pltpu.VMEM((3 * chip, SLOTS, senders), F32),
            pltpu.VMEM((used, senders), F32),
            pltpu.VMEM((hills, LANES), F32),
            pltpu.VMEM((cells, hills), BF16),
            pltpu.VMEM((cells, hills), BF16),
            pltpu.VMEM((hills, depth_bins), BF16),
            pltpu.VMEM((hills, depth_bins), BF16),
        ],
    )
    near = ("z", "c")
    far = ("y", "walk")
    n_near, n_far = lax.axis_size(near), lax.axis_size(far)
    peaks = swap(peak.reshape(n_near, 1, LANES), near).reshape(n_near, LANES)
    peaks = call(spread_max_kernel, "spread", shape_of(n_far, LANES), peaks)
    peaks = swap(peaks.reshape(n_far, 1, LANES), far).reshape(n_far, LANES)
    free = call(free_kernel, "free", shape_of(cells, depth_bins), peaks, new_bias)
    return new_bias.reshape(bias_grid.shape), free.reshape(bias_grid.shape)


def solution(mesh):
    split = Mesh(mesh.devices.reshape(8, 8, 2, mesh.shape["walk"]), EVERY)
    in_specs = (
        P(SLAB, "walk", None),
        P(EVERY, None, None),
        P(EVERY, None),
        P(EVERY, None),
        P(EVERY, None),
        P(EVERY, None),
        P(EVERY),
        P(),
    )
    out_specs = (P(SLAB, "walk", None), P(SLAB, "walk", None))
    return jax.shard_map(
        per_device, mesh=split, in_specs=in_specs, out_specs=out_specs, check_vma=False
    )
```

```python
import functools

import jax
import jax.numpy as jnp
from jax import lax
from jax.experimental import pallas as pl
from jax.experimental.pallas import tpu as pltpu
from jax.sharding import Mesh
from jax.sharding import PartitionSpec as P

SLAB = ("y", "z", "c")
CHIP_ROW = ("c", "walk")
EVERY = SLAB + ("walk",)

BASE_HEIGHT = 1.2
TEMPER = 4.0
SIGMA_SHARE = 0.3125
FREE_SCALE = 10.0 / 9.0

LANES = 128
SLOTS = 4
CHIP = 2
NEAR = 6
FIELD = 32
UNIT = 32
HELD = 64
CHUNK = 256

F32 = jnp.float32
BF16 = jnp.bfloat16
I32 = jnp.int32


def iota(shape, dim, dtype=I32):
    return lax.broadcasted_iota(dtype, shape, dim)


def parts_of(x, count):
    parts = []
    for i in range(count):
        part = x.astype(BF16)
        parts.append(part)
        if i + 1 < count:
            x = x - part.astype(F32)
    return parts


def dot_t(a, b):
    return lax.dot_general(a, b, (((1,), (1,)), ((), ())), preferred_element_type=F32)


def dot(a, b):
    return jnp.dot(a, b, preferred_element_type=F32)


def pack_kernel(rows_dev, *refs):
    arrays, bias, out, bias_out = refs[:7], refs[7], refs[8], refs[9]
    local, sems = refs[10:17], refs[17]
    bias_copy = pltpu.make_async_copy(bias, bias_out, sems.at[len(arrays)])
    copies = [
        pltpu.make_async_copy(a, b, sems.at[i]) for i, (a, b) in enumerate(zip(arrays, local))
    ]
    for c in copies:
        c.start()
    bias_copy.start()
    for c in copies:
        c.wait()
    count, levels, slab, row, col, depth, level = local
    walkers, hills = slab.shape
    chips = out.shape[0]

    def flat(ref):
        return jnp.concatenate([ref[w : w + 1, :] for w in range(walkers)], axis=1)

    total = walkers * hills
    index = iota((1, total), 1)
    limit = jnp.full((1, total), count[0], I32)
    for w in range(1, walkers):
        limit = jnp.where(index < w * hills, limit, count[w] + w * hills)
    target = flat(slab)
    lev = flat(level)
    base = jnp.zeros((1, total), F32)
    for i in range(levels.shape[0]):
        base = jnp.where(lev == i, levels[i], base)
    base = jnp.where(index < limit, BASE_HEIGHT * base, 0.0)
    fields = [
        base,
        (target * rows_dev + flat(row)).astype(F32),
        flat(col).astype(F32),
        flat(depth).astype(F32),
    ]
    line = iota((CHIP * chips, total), 0)
    match = jnp.where(line < chips, CHIP * line, CHIP * (line - chips) + 1) == target
    rank = dot(match.astype(F32).astype(BF16), ahead_of(total))
    rank = jnp.where(match, rank, -1.0)
    place = iota((LANES, total), 0)
    masks, values = [], []
    for slot in range(SLOTS):
        masks.append((rank == slot).astype(F32).astype(BF16))
        value = jnp.zeros((LANES, total), F32)
        for f, field in enumerate(fields):
            value = jnp.where(place == f * FIELD + slot, field, value)
        values.append(value)
    mask = jnp.concatenate(masks, axis=1)
    own = jnp.zeros((CHIP * chips, LANES), F32)
    for part in parts_of(jnp.concatenate(values, axis=1), 3):
        own = own + dot_t(mask, part)
    message = jnp.zeros((chips, LANES), F32)
    for k in range(NEAR):
        part = own[(k % CHIP) * chips : (k % CHIP + 1) * chips, :]
        part = pltpu.roll(part, (1 - k // CHIP) % chips, 0)
        message = message + (pltpu.roll(part, k * SLOTS, 1) if k else part)
    out[...] = message
    bias_copy.wait()


def ahead_of(size):
    return (iota((size, size), 0) < iota((size, size), 1)).astype(F32).astype(BF16)


def numbered(active):
    rows, senders = active.shape
    i, j = iota((rows, rows), 0), iota((rows, rows), 1)
    same = lax.shift_right_logical(i, 2) == lax.shift_right_logical(j, 2)
    chain = (same & (j < i)).astype(F32).astype(BF16)
    earlier = ahead_of(LANES)
    ones = jnp.ones((LANES, LANES), F32).astype(BF16)
    places, counts = [], []
    for b in range(senders // LANES):
        a = active[:, b * LANES : (b + 1) * LANES]
        ab = a.astype(BF16)
        total = dot(ab, ones)
        ahead = dot(chain, total.astype(BF16))
        places.append(jnp.where(a > 0.0, dot(ab, earlier) + ahead, -1.0))
        counts.append(ahead + total)
    return places, counts


def height_kernel(cols_dev, recv, bias, out, table, hi, lo, found):
    senders = recv.shape[0]
    blocks = senders // LANES
    cells, depth_bins = bias.shape
    rows_dev = cells // cols_dev
    walk = lax.axis_index("walk")
    core = lax.axis_index("c")
    for j in range(blocks):
        table[:, j * LANES : (j + 1) * LANES] = recv[j * LANES : (j + 1) * LANES, :].T
    first = CHIP * SLOTS
    rows = CHIP * SLOTS
    base = table[first : first + rows, :]
    row = table[FIELD + first : FIELD + first + rows, :].astype(I32)
    col = table[2 * FIELD + first : 2 * FIELD + first + rows, :].astype(I32)
    depth = table[3 * FIELD + first : 3 * FIELD + first + rows, :]
    col = col - walk * cols_dev
    mine = lax.shift_right_logical(iota(base.shape, 0), 2) == core
    held = mine & (base != 0.0) & (col >= 0) & (col < cols_dev)
    cell = (row & (rows_dev - 1)) * cols_dev + col
    code = (cell * depth_bins).astype(F32) + depth
    place, counts = numbered(held.astype(F32))
    most = jnp.max(functools.reduce(jnp.maximum, counts)).astype(I32)
    hi[...], lo[...] = parts_of(bias[...], 2)
    found[...] = jnp.zeros_like(found)

    def one_pass(t, carry):
        number = (iota((HELD, LANES), 0) + t * HELD).astype(F32)
        codes, hits = [], []
        for j in range(blocks):
            at = slice(j * LANES, (j + 1) * LANES)
            c = jnp.zeros((HELD, LANES), F32)
            for i in range(rows):
                hit = place[j][i : i + 1, :] == number
                hits.append(hit)
                c = jnp.where(hit, code[i : i + 1, at], c)
            codes.append(jnp.sum(c, axis=1, keepdims=True))
        codes = jnp.concatenate(codes, axis=0).astype(I32)
        count = blocks * HELD
        shift = depth_bins.bit_length() - 1
        pick = iota((count, cells), 1) == lax.shift_right_logical(codes, shift)
        pick = pick.astype(F32).astype(BF16)
        lines = dot(pick, hi[...]) + dot(pick, lo[...])
        there = iota((count, depth_bins), 1) == (codes & (depth_bins - 1))
        value = jnp.sum(jnp.where(there, lines, 0.0), axis=1, keepdims=True)
        for j in range(blocks):
            v = value[j * HELD : (j + 1) * HELD, :]
            for i in range(rows):
                back = jnp.sum(jnp.where(hits[j * rows + i], v, 0.0), axis=0, keepdims=True)
                found[i : i + 1, j * LANES : (j + 1) * LANES] += back
        return carry

    lax.fori_loop(0, lax.div(most + (HELD - 1), HELD), one_pass, 0)
    height = jnp.where(held, base * jnp.exp(-found[...] / TEMPER), 0.0)
    for i in range(out.shape[0]):
        out[i] = height


def in_windows(units, offset, count, write):
    for u in range(units):

        def later(t, carry, u=u):
            write(u, t, pl.multiple_of(offset[u] + t * UNIT, 8))
            return carry

        lax.fori_loop(1, lax.div(count[u] + (UNIT - 1), UNIT), later, 0)
    for u in range(units):
        write(u, 0, pl.multiple_of(offset[u], 8))


def gathered(place, field, u, blocks, t):
    number = (iota((UNIT, LANES), 0) + t * UNIT).astype(F32)
    q, j = u // blocks, u % blocks
    at = slice(j * LANES, (j + 1) * LANES)
    found = jnp.zeros((UNIT, LANES), F32)
    for i in range(q * SLOTS, (q + 1) * SLOTS):
        found = jnp.where(place[i : i + 1, at] == number, field[i : i + 1, at], found)
    return jnp.broadcast_to(jnp.sum(found, axis=1, keepdims=True), (UNIT, LANES))


def list_kernel(cols_dev, grid_cols, rows_dev, radius, depth_bins, table, after, codes, place, units, code):
    senders = table.shape[1]
    blocks = senders // LANES
    rows = NEAR * SLOTS
    walk = lax.axis_index("walk")
    core = lax.axis_index("c")
    base = table[0:rows, :]
    row = table[FIELD : FIELD + rows, :].astype(I32)
    col = table[2 * FIELD : 2 * FIELD + rows, :].astype(I32)
    depth = table[3 * FIELD : 3 * FIELD + rows, :].astype(I32)
    line = iota(base.shape, 0)
    col = (col - walk * cols_dev + (radius - 1)) & (grid_cols - 1)
    near = lax.shift_right_logical(line, 2)
    reached = (near >= core) & (near < core + NEAR - 1) & (col < cols_dev + 2 * radius - 1)
    active = reached & (base != 0.0)
    row = near * rows_dev + (row & (rows_dev - 1))
    code[...] = ((row * 256 + col) * depth_bins + depth).astype(F32)
    places, counts = numbered(active.astype(F32))
    for j in range(blocks):
        place[:, j * LANES : (j + 1) * LANES] = places[j]
    total = jnp.int32(0)
    n_units = NEAR * blocks
    for u in range(n_units):
        i = (u // blocks) * SLOTS + SLOTS - 1
        n = jnp.max(counts[u % blocks][i : i + 1, :]).astype(I32)
        units[0, u] = total
        units[1, u] = n
        total = total + ((n + 7) & -8)
    units[0, n_units] = total

    def write(u, t, row):
        codes[pl.ds(row, UNIT), :] = gathered(place, code, u, blocks, t)

    in_windows(n_units, units.at[0], units.at[1], write)


def profile(shifted, radius):
    spread = SIGMA_SHARE * radius
    t = (shifted - radius).astype(F32)
    within = (shifted >= 0) & (shifted < 2 * radius)
    return jnp.where(within, jnp.exp(-(t * t) / (2.0 * spread * spread)), 0.0)


def deposit_kernel(
    rows_dev, cols_dev, radius,
    units, codes, place, below, own, above, bias, out, peak,
    heights, height, row_hi, row_lo, col_hi, col_lo,
):
    blocks = place.shape[1] // LANES
    cells, depth_bins = bias.shape
    core = lax.axis_index("c")
    rows = CHIP * SLOTS
    heights[0:rows, :] = below[...]
    heights[rows : 2 * rows, :] = own[...]
    heights[2 * rows : 3 * rows, :] = above[...]
    n_units = NEAR * blocks

    def write(u, t, row):
        height[pl.ds(row, UNIT), :] = gathered(place, heights, u, blocks, t)

    in_windows(n_units, units.at[0], units.at[1], write)
    total = units[0, n_units]
    out[...] = bias[...]

    def one_chunk(g, carry):
        start = pl.multiple_of(g * CHUNK, CHUNK)
        live = iota((CHUNK, LANES), 0) + start < total
        code = jnp.where(live, codes[pl.ds(start, CHUNK), :], 0.0)
        high = jnp.where(live, height[pl.ds(start, CHUNK), :], 0.0)[:, 0:1]
        depth = code[:, 0:1].astype(I32) & (depth_bins - 1)
        turned = jnp.concatenate(
            [code[i : i + LANES, :].T[0:1, :] for i in range(0, CHUNK, LANES)], axis=1
        ).astype(I32)
        shift = depth_bins.bit_length() - 1
        col = lax.shift_right_logical(turned, shift) & 255
        row = lax.shift_right_logical(turned, shift + 8)
        col_part = profile(iota((cols_dev, CHUNK), 0) - col + (2 * radius - 1), radius)
        for r in range(rows_dev):
            at = slice(r * cols_dev, (r + 1) * cols_dev)
            row_part = profile((core + CHIP) * rows_dev + r - row + radius, radius)
            row_hi[at, :], row_lo[at, :] = parts_of(col_part * row_part, 2)
        around = (iota((CHUNK, depth_bins), 1) - depth + radius) & (depth_bins - 1)
        col_hi[...], col_lo[...] = parts_of(profile(around, radius) * high, 2)
        added = dot(row_hi[...], col_lo[...]) + dot(row_lo[...], col_hi[...])
        out[...] += added + dot(row_hi[...], col_hi[...])
        return carry

    lax.fori_loop(0, lax.div(total + (CHUNK - 1), CHUNK), one_chunk, 0)
    peak[...] = jnp.full(peak.shape, jnp.max(out[...]), F32)


def spread_max_kernel(recv, out):
    out[...] = jnp.full(out.shape, jnp.max(recv[...]), F32)


def free_kernel(recv, bias, out):
    out[...] = FREE_SCALE * (jnp.max(recv[...]) - bias[...])


def call(body, name, out_shape, *operands, smem=0, space=pltpu.VMEM, scratch=()):
    spaces = [pltpu.SMEM if i < smem else space for i in range(len(operands))]
    operands = [
        x if i < smem else pltpu.with_memory_space_constraint(x, space)
        for i, x in enumerate(operands)
    ]
    out_specs = jax.tree.map(
        lambda s: pl.BlockSpec(
            memory_space=pltpu.SMEM if getattr(s, "dtype", None) == I32 else pltpu.VMEM
        ),
        out_shape,
    )
    return pl.pallas_call(
        body,
        name=name,
        out_shape=out_shape,
        in_specs=[pl.BlockSpec(memory_space=m) for m in spaces],
        out_specs=out_specs,
        scratch_shapes=list(scratch),
        compiler_params=pltpu.CompilerParams(vmem_limit_bytes=24 << 20),
    )(*operands)


def vmem(*dims):
    return pltpu.VMEM(dims, F32)


def hbm(*dims):
    return jax.ShapeDtypeStruct(dims, F32)


def swap(array, axes):
    return lax.all_to_all(array, axes, 0, 0, tiled=True)


def copied(array, axes):
    return swap(jnp.broadcast_to(array[None], (lax.axis_size(axes), *array.shape)), axes)


def per_device(
    bias_grid, hill_slab, hill_row, hill_col, hill_depth, hill_level, hill_count, height_levels
):
    rows_dev, cols_dev, depth_bins = bias_grid.shape
    n_slab = lax.axis_size(SLAB)
    n_walk = lax.axis_size("walk")
    radius = 2 * rows_dev
    grid_cols = cols_dev * n_walk
    senders = n_slab * n_walk
    cells = rows_dev * cols_dev
    chips = n_slab // CHIP
    blocks = senders // LANES
    rows = NEAR * SLOTS

    message, bias = call(
        functools.partial(pack_kernel, rows_dev),
        "pack",
        (vmem(chips, LANES), vmem(cells, depth_bins)),
        hill_count,
        height_levels,
        hill_slab[:, :, 0],
        hill_row,
        hill_col,
        hill_depth,
        hill_level,
        bias_grid.reshape(cells, depth_bins),
        space=pltpu.HBM,
        scratch=[pltpu.SMEM(hill_count.shape, I32), pltpu.SMEM(height_levels.shape, F32)]
        + [pltpu.VMEM(hill_row.shape, I32)] * 5
        + [pltpu.SemaphoreType.DMA((8,))],
    )
    message = swap(message.reshape(chips, 1, LANES), ("y", "z")).reshape(chips, LANES)
    recv = copied(message, CHIP_ROW).reshape(senders, LANES)

    own, table = call(
        functools.partial(height_kernel, cols_dev),
        "heights",
        (vmem(CHIP * n_walk, CHIP * SLOTS, senders), vmem(LANES, senders)),
        recv,
        bias,
        scratch=[pltpu.VMEM((cells, depth_bins), BF16)] * 2
        + [pltpu.VMEM((CHIP * SLOTS, senders), F32)],
    )
    own = swap(own, CHIP_ROW).sum(axis=0)
    ring = range(n_slab)
    below = lax.ppermute(own, SLAB, [(s, (s + CHIP) % n_slab) for s in ring])
    above = lax.ppermute(own, SLAB, [(s, (s - CHIP) % n_slab) for s in ring])

    most = (NEAR - 1) * SLOTS * senders + 8 * NEAR * blocks + UNIT
    most = -(-most // CHUNK) * CHUNK
    codes, place, units = call(
        functools.partial(list_kernel, cols_dev, grid_cols, rows_dev, radius, depth_bins),
        "list",
        (vmem(most, LANES), vmem(rows, senders), jax.ShapeDtypeStruct((2, LANES), I32)),
        table,
        own,
        scratch=[pltpu.VMEM((rows, senders), F32)],
    )
    near, far = ("z", "c"), ("y", "walk")
    n_near, n_far = lax.axis_size(near), lax.axis_size(far)
    new_bias, peak = call(
        functools.partial(deposit_kernel, rows_dev, cols_dev, radius),
        "deposit",
        (vmem(cells, depth_bins), vmem(n_near, LANES)),
        units,
        codes,
        place,
        below,
        own,
        above,
        bias,
        smem=1,
        scratch=[
            pltpu.VMEM((rows, senders), F32),
            pltpu.VMEM((most, LANES), F32),
            pltpu.VMEM((cells, CHUNK), BF16),
            pltpu.VMEM((cells, CHUNK), BF16),
            pltpu.VMEM((CHUNK, depth_bins), BF16),
            pltpu.VMEM((CHUNK, depth_bins), BF16),
        ],
    )
    peaks = swap(peak.reshape(n_near, 1, LANES), near).reshape(n_near, LANES)
    peaks = call(spread_max_kernel, "spread", vmem(n_far, LANES), peaks)
    peaks = swap(peaks.reshape(n_far, 1, LANES), far).reshape(n_far, LANES)
    free = call(free_kernel, "free", hbm(cells, depth_bins), peaks, new_bias)
    return new_bias.reshape(bias_grid.shape), free.reshape(bias_grid.shape)


def solution(mesh):
    split = Mesh(mesh.devices.reshape(8, 8, 2, mesh.shape["walk"]), EVERY)
    in_specs = (
        P(SLAB, "walk", None),
        P(EVERY, None, None),
        P(EVERY, None),
        P(EVERY, None),
        P(EVERY, None),
        P(EVERY, None),
        P(EVERY),
        P(),
    )
    out_specs = (P(SLAB, "walk", None), P(SLAB, "walk", None))
    return jax.shard_map(
        per_device, mesh=split, in_specs=in_specs, out_specs=out_specs, check_vma=False
    )
```

```python
import functools
import math

import jax
import jax.numpy as jnp
from jax import lax
from jax.experimental import pallas as pl
from jax.experimental.pallas import tpu as pltpu
from jax.sharding import Mesh
from jax.sharding import PartitionSpec as P

SLAB = ("y", "zh", "zl", "c")
CHIP_ROW = ("c", "walk")
QUAD = ("zl", "c", "walk")
EVERY = SLAB + ("walk",)

BASE_HEIGHT = 1.2
TEMPER = 4.0
SIGMA_SHARE = 0.3125
FREE_SCALE = 10.0 / 9.0

LANES = 128
SLOTS = 4
CHIP = 2
NEAR = 6
FIELD = 32
UNIT = 32
LATER = 64
HELD = 96
CHUNK = 256
STRIPS = 4
AHEAD = 4

F32 = jnp.float32
BF16 = jnp.bfloat16
I32 = jnp.int32


def iota(shape, dim, dtype=I32):
    return lax.broadcasted_iota(dtype, shape, dim)


def parts_of(x, count):
    parts = []
    for i in range(count):
        part = x.astype(BF16)
        parts.append(part)
        if i + 1 < count:
            x = x - part.astype(F32)
    return parts


def dot_t(a, b):
    return lax.dot_general(a, b, (((1,), (1,)), ((), ())), preferred_element_type=F32)


def dot(a, b):
    return jnp.dot(a, b, preferred_element_type=F32)


def pack_kernel(rows_dev, *refs):
    arrays, bias, out, bias_out = refs[:7], refs[7], refs[8], refs[9]
    local, sems = refs[10:17], refs[17]
    bias_copy = pltpu.make_async_copy(bias, bias_out, sems.at[len(arrays)])
    copies = [
        pltpu.make_async_copy(a, b, sems.at[i]) for i, (a, b) in enumerate(zip(arrays, local))
    ]
    for c in copies:
        c.start()
    bias_copy.start()
    for c in copies:
        c.wait()
    count, levels, slab, row, col, depth, level = local
    walkers, hills = slab.shape
    chips = out.shape[0]

    def flat(ref):
        return jnp.concatenate([ref[w : w + 1, :] for w in range(walkers)], axis=1)

    total = walkers * hills
    index = iota((1, total), 1)
    limit = jnp.full((1, total), count[0], I32)
    for w in range(1, walkers):
        limit = jnp.where(index < w * hills, limit, count[w] + w * hills)
    target = flat(slab)
    lev = flat(level)
    base = jnp.zeros((1, total), F32)
    for i in range(levels.shape[0]):
        base = jnp.where(lev == i, levels[i], base)
    base = jnp.where(index < limit, BASE_HEIGHT * base, 0.0)
    fields = [
        base,
        (target * rows_dev + flat(row)).astype(F32),
        flat(col).astype(F32),
        flat(depth).astype(F32),
    ]
    line = iota((CHIP * chips, total), 0)
    match = jnp.where(line < chips, CHIP * line, CHIP * (line - chips) + 1) == target
    rank = dot(match.astype(F32).astype(BF16), ahead_of(total))
    rank = jnp.where(match, rank, -1.0)
    place = iota((LANES, total), 0)
    masks, values = [], []
    for slot in range(SLOTS):
        masks.append((rank == slot).astype(F32).astype(BF16))
        value = jnp.zeros((LANES, total), F32)
        for f, field in enumerate(fields):
            value = jnp.where(place == f * FIELD + slot, field, value)
        values.append(value)
    mask = jnp.concatenate(masks, axis=1)
    own = jnp.zeros((CHIP * chips, LANES), F32)
    for part in parts_of(jnp.concatenate(values, axis=1), 3):
        own = own + dot_t(mask, part)
    message = jnp.zeros((chips, LANES), F32)
    for k in range(NEAR):
        part = own[(k % CHIP) * chips : (k % CHIP + 1) * chips, :]
        part = pltpu.roll(part, (1 - k // CHIP) % chips, 0)
        message = message + (pltpu.roll(part, k * SLOTS, 1) if k else part)
    out[...] = message
    bias_copy.wait()


def ahead_of(size):
    return (iota((size, size), 0) < iota((size, size), 1)).astype(F32).astype(BF16)


def numbered(active):
    rows, senders = active.shape
    i, j = iota((rows, rows), 0), iota((rows, rows), 1)
    same = lax.shift_right_logical(i, 2) == lax.shift_right_logical(j, 2)
    chain = (same & (j < i)).astype(F32).astype(BF16)
    earlier = ahead_of(LANES)
    ones = jnp.ones((LANES, LANES), F32).astype(BF16)
    places, counts = [], []
    for b in range(senders // LANES):
        a = active[:, b * LANES : (b + 1) * LANES]
        ab = a.astype(BF16)
        total = dot(ab, ones)
        ahead = dot(chain, total.astype(BF16))
        places.append(jnp.where(a > 0.0, dot(ab, earlier) + ahead, -1.0))
        counts.append(ahead + total)
    return places, counts


def height_kernel(cols_dev, recv, bias, out, table, hi, lo, found):
    senders = recv.shape[0]
    blocks = senders // LANES
    cells, depth_bins = bias.shape
    rows_dev = cells // cols_dev
    walk = lax.axis_index("walk")
    core = lax.axis_index("c")
    for j in range(blocks):
        table[:, j * LANES : (j + 1) * LANES] = recv[j * LANES : (j + 1) * LANES, :].T
    first = CHIP * SLOTS
    rows = CHIP * SLOTS
    base = table[first : first + rows, :]
    row = table[FIELD + first : FIELD + first + rows, :].astype(I32)
    col = table[2 * FIELD + first : 2 * FIELD + first + rows, :].astype(I32)
    depth = table[3 * FIELD + first : 3 * FIELD + first + rows, :]
    col = col - walk * cols_dev
    mine = lax.shift_right_logical(iota(base.shape, 0), 2) == core
    held = mine & (base != 0.0) & (col >= 0) & (col < cols_dev)
    cell = (row & (rows_dev - 1)) * cols_dev + col
    code = (cell * depth_bins).astype(F32) + depth
    place, counts = numbered(held.astype(F32))
    most = jnp.max(functools.reduce(jnp.maximum, counts)).astype(I32)
    hi[...], lo[...] = parts_of(bias[...], 2)
    found[...] = jnp.zeros_like(found)

    def one_pass(t, carry):
        number = (iota((HELD, LANES), 0) + t * HELD).astype(F32)
        codes, hits = [], []
        for j in range(blocks):
            at = slice(j * LANES, (j + 1) * LANES)
            c = jnp.zeros((HELD, LANES), F32)
            for i in range(rows):
                hit = place[j][i : i + 1, :] == number
                hits.append(hit)
                c = jnp.where(hit, code[i : i + 1, at], c)
            codes.append(jnp.sum(c, axis=1, keepdims=True))
        codes = jnp.concatenate(codes, axis=0).astype(I32)
        count = blocks * HELD
        shift = depth_bins.bit_length() - 1
        pick = iota((count, cells), 1) == lax.shift_right_logical(codes, shift)
        pick = pick.astype(F32).astype(BF16)
        lines = dot(pick, hi[...]) + dot(pick, lo[...])
        there = iota((count, depth_bins), 1) == (codes & (depth_bins - 1))
        value = jnp.sum(jnp.where(there, lines, 0.0), axis=1, keepdims=True)
        for j in range(blocks):
            v = value[j * HELD : (j + 1) * HELD, :]
            for i in range(rows):
                back = jnp.sum(jnp.where(hits[j * rows + i], v, 0.0), axis=0, keepdims=True)
                found[i : i + 1, j * LANES : (j + 1) * LANES] += back
        return carry

    lax.fori_loop(0, lax.div(most + (HELD - 1), HELD), one_pass, 0)
    height = jnp.where(held, base * jnp.exp(-found[...] / TEMPER), 0.0)
    height = height[:SLOTS, :] + height[SLOTS:, :]
    for i in range(out.shape[0]):
        out[i] = height


def in_windows(units, offset, count, write):
    for u in range(units):

        def later(t, carry, u=u):
            first = UNIT + t * LATER
            write(u, first, LATER, offset[u] + first)
            return carry

        lax.fori_loop(0, lax.div(count[u] + (LATER - 1 - UNIT), LATER), later, 0)
    for u in range(units):
        write(u, 0, UNIT, offset[u])


def gathered(place, field, u, blocks, first, rows):
    number = (iota((rows, LANES), 0) + first).astype(F32)
    q, j = u // blocks, u % blocks
    at = slice(j * LANES, (j + 1) * LANES)
    found = jnp.zeros((rows, LANES), F32)
    for i in range(q * SLOTS, (q + 1) * SLOTS):
        found = jnp.where(place[i : i + 1, at] == number, field[i : i + 1, at], found)
    return jnp.broadcast_to(jnp.sum(found, axis=1, keepdims=True), (rows, LANES))


def list_kernel(
    cols_dev, grid_cols, rows_dev, radius, depth_bins,
    table, after, codes, place, units, planes, lines, code,
):
    senders = table.shape[1]
    blocks = senders // LANES
    rows = NEAR * SLOTS
    walk = lax.axis_index("walk")
    core = lax.axis_index("c")
    base = table[0:rows, :]
    row = table[FIELD : FIELD + rows, :].astype(I32)
    col = table[2 * FIELD : 2 * FIELD + rows, :].astype(I32)
    depth = table[3 * FIELD : 3 * FIELD + rows, :].astype(I32)
    line = iota(base.shape, 0)
    col = (col - walk * cols_dev + (radius - 1)) & (grid_cols - 1)
    near = lax.shift_right_logical(line, 2)
    reached = (near >= core) & (near < core + NEAR - 1) & (col < cols_dev + 2 * radius - 1)
    row = near * rows_dev + (row & (rows_dev - 1))
    active = reached & (base != 0.0) & (row > core * rows_dev)
    code[...] = ((row * 256 + col) * depth_bins + depth).astype(F32)
    places, counts = numbered(active.astype(F32))
    for j in range(blocks):
        place[:, j * LANES : (j + 1) * LANES] = places[j]
    total = jnp.int32(0)
    n_units = NEAR * blocks
    for u in range(n_units):
        i = (u // blocks) * SLOTS + SLOTS - 1
        n = jnp.max(counts[u % blocks][i : i + 1, :]).astype(I32)
        units[0, u] = total
        units[1, u] = n
        total = total + n
    units[0, n_units] = total

    def write(u, first, size, row):
        codes[pl.ds(row, size), :] = gathered(place, code, u, blocks, first, size)

    in_windows(n_units, units.at[0], units.at[1], write)

    def ahead(g, carry):
        listed = live_rows(codes, pl.multiple_of(g * CHUNK, CHUNK), total)
        factors(
            listed, core, rows_dev, cols_dev, depth_bins, radius, planes.at[g], lines.at[g]
        )
        return carry

    lax.fori_loop(0, jnp.minimum(chunks_of(total), AHEAD), ahead, 0)


def profile(shifted, radius, wrapped=False):
    spread = SIGMA_SHARE * radius
    t = shifted.astype(F32) - radius
    within = shifted < 2 * radius
    if not wrapped:
        within = within & (shifted >= 0)
    return jnp.where(within, jnp.exp2(t * t * (-math.log2(math.e) / (2.0 * spread**2))), 0.0)


def factors(code, core, rows_dev, cols_dev, depth_bins, radius, planes, lines):
    depth = code[:, 0:1].astype(I32) & (depth_bins - 1)
    around = (iota((CHUNK, depth_bins), 1) + (radius - depth)) & (depth_bins - 1)
    lines[...] = profile(around, radius, wrapped=True)
    turned = jnp.concatenate(
        [code[i : i + LANES, :].T[0:1, :] for i in range(0, CHUNK, LANES)], axis=1
    ).astype(I32)
    shift = depth_bins.bit_length() - 1
    col = lax.shift_right_logical(turned, shift) & 255
    row = lax.shift_right_logical(turned, shift + 8)
    col_part = profile(iota((cols_dev, CHUNK), 0) - col + (2 * radius - 1), radius)
    for r in range(rows_dev):
        at = slice(r * cols_dev, (r + 1) * cols_dev)
        row_part = profile((core + CHIP) * rows_dev + r - row + radius, radius)
        hi, lo = parts_of(col_part * row_part, 2)
        planes[at, 0:CHUNK] = hi
        planes[at, CHUNK : 2 * CHUNK] = hi
        planes[at, 2 * CHUNK : 3 * CHUNK] = lo


def live_rows(array, start, total):
    live = iota((CHUNK, LANES), 0) + start < total
    return jnp.where(live, array[pl.ds(start, CHUNK), :], 0.0)


def chunks_of(total):
    return lax.div(total + (CHUNK - 1), CHUNK)


def deposit_kernel(
    rows_dev, cols_dev, radius,
    units, codes, place, planes, lines, quad, edge, bias, out, peak,
    heights, height, more_planes, more_lines, scaled,
):
    blocks = place.shape[1] // LANES
    depth_bins = bias.shape[1]
    core = lax.axis_index("c")
    lower = lax.axis_index("zl") == 0
    for k in range(CHIP):
        parts = edge[CHIP + k], quad[k], quad[CHIP + k], edge[k]
        for i in range(NEAR // CHIP):
            at = (i * CHIP + k) * SLOTS
            heights[at : at + SLOTS, :] = jnp.where(lower, parts[i], parts[i + 1])
    n_units = NEAR * blocks

    def write(u, first, size, row):
        height[pl.ds(row, size), :] = gathered(place, heights, u, blocks, first, size)

    in_windows(n_units, units.at[0], units.at[1], write)
    total = units[0, n_units]
    out[...] = bias[...]

    def add(g, plane, line):
        high = live_rows(height, pl.multiple_of(g * CHUNK, CHUNK), total)[:, 0:1]
        hi, lo = parts_of(line * high, 2)
        scaled[0:CHUNK, :] = hi
        scaled[CHUNK : 2 * CHUNK, :] = lo
        scaled[2 * CHUNK : 3 * CHUNK, :] = hi
        out[...] += dot(plane, scaled[...])

    def ready(g, carry):
        add(g, planes[g], lines[g])
        return carry

    def rest(g, carry):
        code = live_rows(codes, pl.multiple_of(g * CHUNK, CHUNK), total)
        factors(code, core, rows_dev, cols_dev, depth_bins, radius, more_planes, more_lines)
        add(g, more_planes[...], more_lines[...])
        return carry

    count = chunks_of(total)
    lax.fori_loop(0, jnp.minimum(count, AHEAD), ready, 0)
    lax.fori_loop(AHEAD, count, rest, 0)
    peak[...] = jnp.full(peak.shape, jnp.max(out[...]), F32)


def free_kernel(recv, bias, bias_out, out, free, sems):
    bias_copy = pltpu.make_async_copy(bias, bias_out, sems.at[STRIPS])
    bias_copy.start()
    highest = jnp.max(recv[...])
    size = bias.shape[0] // STRIPS
    copies = []
    for i in range(STRIPS):
        at = pl.ds(i * size, size)
        free[at, :] = FREE_SCALE * (highest - bias[at, :])
        copies.append(pltpu.make_async_copy(free.at[at, :], out.at[at, :], sems.at[i]))
        copies[-1].start()
    for c in copies:
        c.wait()
    bias_copy.wait()


def call(body, name, out_shape, *operands, smem=0, space=pltpu.VMEM, scratch=()):
    spaces = [pltpu.SMEM if i < smem else space for i in range(len(operands))]
    operands = [
        x if i < smem else pltpu.with_memory_space_constraint(x, space)
        for i, x in enumerate(operands)
    ]
    def space_of(shape):
        if isinstance(shape, jax.ShapeDtypeStruct):
            return pltpu.SMEM if shape.dtype == I32 else pltpu.HBM
        return pltpu.VMEM

    out_specs = jax.tree.map(lambda s: pl.BlockSpec(memory_space=space_of(s)), out_shape)
    return pl.pallas_call(
        body,
        name=name,
        out_shape=out_shape,
        in_specs=[pl.BlockSpec(memory_space=m) for m in spaces],
        out_specs=out_specs,
        scratch_shapes=list(scratch),
        compiler_params=pltpu.CompilerParams(vmem_limit_bytes=24 << 20),
    )(*operands)


def vmem(*dims):
    return pltpu.VMEM(dims, F32)


def hbm(*dims):
    return jax.ShapeDtypeStruct(dims, F32)


def swap(array, axes):
    return lax.all_to_all(array, axes, 0, 0, tiled=True)


def copied(array, axes):
    return swap(jnp.broadcast_to(array[None], (lax.axis_size(axes), *array.shape)), axes)


def per_device(
    bias_grid, hill_slab, hill_row, hill_col, hill_depth, hill_level, hill_count, height_levels
):
    rows_dev, cols_dev, depth_bins = bias_grid.shape
    n_slab = lax.axis_size(SLAB)
    n_walk = lax.axis_size("walk")
    radius = 2 * rows_dev
    grid_cols = cols_dev * n_walk
    senders = n_slab * n_walk
    cells = rows_dev * cols_dev
    chips = n_slab // CHIP
    blocks = senders // LANES
    rows = NEAR * SLOTS
    quads = 2 * CHIP

    message, bias = call(
        functools.partial(pack_kernel, rows_dev),
        "pack",
        (vmem(chips, LANES), vmem(cells, depth_bins)),
        hill_count,
        height_levels,
        hill_slab[:, :, 0],
        hill_row,
        hill_col,
        hill_depth,
        hill_level,
        bias_grid.reshape(cells, depth_bins),
        space=pltpu.HBM,
        scratch=[pltpu.SMEM(hill_count.shape, I32), pltpu.SMEM(height_levels.shape, F32)]
        + [pltpu.VMEM(hill_row.shape, I32)] * 5
        + [pltpu.SemaphoreType.DMA((8,))],
    )
    message = swap(message.reshape(chips, 1, LANES), ("y", "zh", "zl")).reshape(chips, LANES)
    recv = copied(message, CHIP_ROW).reshape(senders, LANES)

    own, table = call(
        functools.partial(height_kernel, cols_dev),
        "heights",
        (vmem(quads * n_walk, SLOTS, senders), vmem(LANES, senders)),
        recv,
        bias,
        scratch=[pltpu.VMEM((cells, depth_bins), BF16)] * 2
        + [pltpu.VMEM((CHIP * SLOTS, senders), F32)],
    )
    quad = swap(own, QUAD).reshape(quads, n_walk, SLOTS, senders).sum(axis=1)
    route = [(s, (s + (CHIP if s % quads >= CHIP else -CHIP)) % n_slab) for s in range(n_slab)]
    edge = lax.ppermute(quad, SLAB, route)

    most = (NEAR - 1) * SLOTS * senders + LATER
    most = -(-most // CHUNK) * CHUNK
    codes, place, units, planes, lines = call(
        functools.partial(list_kernel, cols_dev, grid_cols, rows_dev, radius, depth_bins),
        "list",
        (
            vmem(most, LANES),
            vmem(rows, senders),
            jax.ShapeDtypeStruct((2, LANES), I32),
            pltpu.VMEM((AHEAD, cells, 3 * CHUNK), BF16),
            vmem(AHEAD, CHUNK, depth_bins),
        ),
        table,
        quad,
        scratch=[pltpu.VMEM((rows, senders), F32)],
    )
    near, far = ("zh", "zl", "c"), ("y", "walk")
    n_near, n_far = lax.axis_size(near), lax.axis_size(far)
    new_bias, peak = call(
        functools.partial(deposit_kernel, rows_dev, cols_dev, radius),
        "deposit",
        (vmem(cells, depth_bins), vmem(n_near, LANES)),
        units,
        codes,
        place,
        planes,
        lines,
        quad,
        edge,
        bias,
        smem=1,
        scratch=[
            pltpu.VMEM((rows, senders), F32),
            pltpu.VMEM((most, LANES), F32),
            pltpu.VMEM((cells, 3 * CHUNK), BF16),
            pltpu.VMEM((CHUNK, depth_bins), F32),
            pltpu.VMEM((3 * CHUNK, depth_bins), BF16),
        ],
    )
    peaks = swap(peak.reshape(n_near, 1, LANES), near).max(axis=0)
    peaks = swap(jnp.broadcast_to(peaks, (n_far, 1, LANES)), far).reshape(n_far, LANES)
    new_bias, free = call(
        free_kernel,
        "free",
        (hbm(cells, depth_bins), hbm(cells, depth_bins)),
        peaks,
        new_bias,
        scratch=[
            pltpu.VMEM((cells, depth_bins), F32),
            pltpu.SemaphoreType.DMA((STRIPS + 1,)),
        ],
    )
    return new_bias.reshape(bias_grid.shape), free.reshape(bias_grid.shape)


def solution(mesh):
    split = Mesh(mesh.devices.reshape(8, 4, 2, 2, mesh.shape["walk"]), EVERY)
    in_specs = (
        P(SLAB, "walk", None),
        P(EVERY, None, None),
        P(EVERY, None),
        P(EVERY, None),
        P(EVERY, None),
        P(EVERY, None),
        P(EVERY),
        P(),
    )
    out_specs = (P(SLAB, "walk", None), P(SLAB, "walk", None))
    return jax.shard_map(
        per_device, mesh=split, in_specs=in_specs, out_specs=out_specs, check_vma=False
    )
```

```python
import functools
import math

import jax
import jax.numpy as jnp
from jax import lax
from jax.experimental import pallas as pl
from jax.experimental.pallas import tpu as pltpu
from jax.sharding import Mesh
from jax.sharding import PartitionSpec as P

SLAB = ("y", "zh", "zl", "c")
CHIP_ROW = ("c", "walk")
QUAD = ("zl", "c", "walk")
EVERY = SLAB + ("walk",)

BASE_HEIGHT = 1.2
TEMPER = 4.0
SIGMA_SHARE = 0.3125
FREE_SCALE = 10.0 / 9.0

LANES = 128
SLOTS = 4
CHIP = 2
NEAR = 6
FIELD = 32
UNIT = 32
LATER = 64
HELD = 96
CHUNK = 256
STRIPS = 4
AHEAD = 4

F32 = jnp.float32
BF16 = jnp.bfloat16
I32 = jnp.int32


def iota(shape, dim, dtype=I32):
    return lax.broadcasted_iota(dtype, shape, dim)


def parts_of(x, count):
    parts = []
    for i in range(count):
        part = x.astype(BF16)
        parts.append(part)
        if i + 1 < count:
            x = x - part.astype(F32)
    return parts


def dot_t(a, b):
    return lax.dot_general(a, b, (((1,), (1,)), ((), ())), preferred_element_type=F32)


def dot(a, b):
    return jnp.dot(a, b, preferred_element_type=F32)


def pack_kernel(rows_dev, *refs):
    arrays, bias, out, bias_out = refs[:7], refs[7], refs[8], refs[9]
    local, sems = refs[10:17], refs[17]
    bias_copy = pltpu.make_async_copy(bias, bias_out, sems.at[len(arrays)])
    copies = [
        pltpu.make_async_copy(a, b, sems.at[i]) for i, (a, b) in enumerate(zip(arrays, local))
    ]
    for c in copies:
        c.start()
    bias_copy.start()
    for c in copies:
        c.wait()
    count, levels, slab, row, col, depth, level = local
    walkers, hills = slab.shape
    chips = out.shape[0]

    def flat(ref):
        return jnp.concatenate([ref[w : w + 1, :] for w in range(walkers)], axis=1)

    total = walkers * hills
    index = iota((1, total), 1)
    limit = jnp.full((1, total), count[0], I32)
    for w in range(1, walkers):
        limit = jnp.where(index < w * hills, limit, count[w] + w * hills)
    target = flat(slab)
    lev = flat(level)
    base = jnp.zeros((1, total), F32)
    for i in range(levels.shape[0]):
        base = jnp.where(lev == i, levels[i], base)
    base = jnp.where(index < limit, BASE_HEIGHT * base, 0.0)
    fields = [
        base,
        (target * rows_dev + flat(row)).astype(F32),
        flat(col).astype(F32),
        flat(depth).astype(F32),
    ]
    line = iota((CHIP * chips, total), 0)
    match = jnp.where(line < chips, CHIP * line, CHIP * (line - chips) + 1) == target
    rank = dot(match.astype(F32).astype(BF16), ahead_of(total))
    rank = jnp.where(match, rank, -1.0)
    place = iota((LANES, total), 0)
    masks, values = [], []
    for slot in range(SLOTS):
        masks.append((rank == slot).astype(F32).astype(BF16))
        value = jnp.zeros((LANES, total), F32)
        for f, field in enumerate(fields):
            value = jnp.where(place == f * FIELD + slot, field, value)
        values.append(value)
    mask = jnp.concatenate(masks, axis=1)
    own = jnp.zeros((CHIP * chips, LANES), F32)
    for part in parts_of(jnp.concatenate(values, axis=1), 3):
        own = own + dot_t(mask, part)
    message = jnp.zeros((chips, LANES), F32)
    for k in range(NEAR):
        part = own[(k % CHIP) * chips : (k % CHIP + 1) * chips, :]
        part = pltpu.roll(part, (1 - k // CHIP) % chips, 0)
        message = message + (pltpu.roll(part, k * SLOTS, 1) if k else part)
    out[...] = message
    bias_copy.wait()


def ahead_of(size):
    return (iota((size, size), 0) < iota((size, size), 1)).astype(F32).astype(BF16)


def numbered(active):
    rows, senders = active.shape
    i, j = iota((rows, rows), 0), iota((rows, rows), 1)
    same = lax.shift_right_logical(i, 2) == lax.shift_right_logical(j, 2)
    chain = (same & (j < i)).astype(F32).astype(BF16)
    earlier = ahead_of(LANES)
    ones = jnp.ones((LANES, LANES), F32).astype(BF16)
    places, counts = [], []
    for b in range(senders // LANES):
        a = active[:, b * LANES : (b + 1) * LANES]
        ab = a.astype(BF16)
        total = dot(ab, ones)
        ahead = dot(chain, total.astype(BF16))
        places.append(jnp.where(a > 0.0, dot(ab, earlier) + ahead, -1.0))
        counts.append(ahead + total)
    return places, counts


def height_kernel(cols_dev, recv, bias, out, table, hi, lo, found):
    senders = recv.shape[0]
    blocks = senders // LANES
    cells, depth_bins = bias.shape
    rows_dev = cells // cols_dev
    walk = lax.axis_index("walk")
    core = lax.axis_index("c")
    for j in range(blocks):
        table[:, j * LANES : (j + 1) * LANES] = recv[j * LANES : (j + 1) * LANES, :].T
    first = CHIP * SLOTS
    rows = CHIP * SLOTS
    base = table[first : first + rows, :]
    row = table[FIELD + first : FIELD + first + rows, :].astype(I32)
    col = table[2 * FIELD + first : 2 * FIELD + first + rows, :].astype(I32)
    depth = table[3 * FIELD + first : 3 * FIELD + first + rows, :]
    col = col - walk * cols_dev
    mine = lax.shift_right_logical(iota(base.shape, 0), 2) == core
    held = mine & (base != 0.0) & (col >= 0) & (col < cols_dev)
    cell = (row & (rows_dev - 1)) * cols_dev + col
    code = (cell * depth_bins).astype(F32) + depth
    place, counts = numbered(held.astype(F32))
    most = jnp.max(functools.reduce(jnp.maximum, counts)).astype(I32)
    hi[...], lo[...] = parts_of(bias[...], 2)
    found[...] = jnp.zeros_like(found)

    def one_pass(t, carry):
        number = (iota((HELD, LANES), 0) + t * HELD).astype(F32)
        codes, hits = [], []
        for j in range(blocks):
            at = slice(j * LANES, (j + 1) * LANES)
            c = jnp.zeros((HELD, LANES), F32)
            for i in range(rows):
                hit = place[j][i : i + 1, :] == number
                hits.append(hit)
                c = jnp.where(hit, code[i : i + 1, at], c)
            codes.append(jnp.sum(c, axis=1, keepdims=True))
        codes = jnp.concatenate(codes, axis=0).astype(I32)
        count = blocks * HELD
        shift = depth_bins.bit_length() - 1
        pick = iota((count, cells), 1) == lax.shift_right_logical(codes, shift)
        pick = pick.astype(F32).astype(BF16)
        lines = dot(pick, hi[...]) + dot(pick, lo[...])
        there = iota((count, depth_bins), 1) == (codes & (depth_bins - 1))
        value = jnp.sum(jnp.where(there, lines, 0.0), axis=1, keepdims=True)
        for j in range(blocks):
            v = value[j * HELD : (j + 1) * HELD, :]
            for i in range(rows):
                back = jnp.sum(jnp.where(hits[j * rows + i], v, 0.0), axis=0, keepdims=True)
                found[i : i + 1, j * LANES : (j + 1) * LANES] += back
        return carry

    lax.fori_loop(0, lax.div(most + (HELD - 1), HELD), one_pass, 0)
    height = jnp.where(held, base * jnp.exp(-found[...] / TEMPER), 0.0)
    height = height[:SLOTS, :] + height[SLOTS:, :]
    for i in range(out.shape[0]):
        out[i] = height


def in_windows(blocks, offset, count, write):
    units = NEAR * blocks

    @pl.when(count[units] > UNIT)
    def _():
        for q in range(NEAR):
            some = range(q * blocks, (q + 1) * blocks)
            most = functools.reduce(jnp.maximum, [count[u] for u in some])
            times = lax.div(most + (LATER - 1 - UNIT), LATER)

            def later(t, carry, some=some, times=times):
                first = UNIT + (times - 1 - t) * LATER
                for u in some:
                    write(u, first, LATER, offset[u] + first)
                return carry

            lax.fori_loop(0, times, later, 0)

    for u in range(units):
        write(u, 0, UNIT, offset[u])


def gathered(place, field, u, blocks, first, rows):
    number = (iota((rows, LANES), 0) + first).astype(F32)
    q, j = u // blocks, u % blocks
    at = slice(j * LANES, (j + 1) * LANES)
    found = jnp.zeros((rows, LANES), F32)
    for i in range(q * SLOTS, (q + 1) * SLOTS):
        found = jnp.where(place[i : i + 1, at] == number, field[i : i + 1, at], found)
    return jnp.broadcast_to(jnp.sum(found, axis=1, keepdims=True), (rows, LANES))


def list_kernel(
    cols_dev, grid_cols, rows_dev, radius, depth_bins,
    table, after, codes, place, units, planes, lines, code,
):
    senders = table.shape[1]
    blocks = senders // LANES
    rows = NEAR * SLOTS
    walk = lax.axis_index("walk")
    core = lax.axis_index("c")
    base = table[0:rows, :]
    row = table[FIELD : FIELD + rows, :].astype(I32)
    col = table[2 * FIELD : 2 * FIELD + rows, :].astype(I32)
    depth = table[3 * FIELD : 3 * FIELD + rows, :].astype(I32)
    line = iota(base.shape, 0)
    col = (col - walk * cols_dev + (radius - 1)) & (grid_cols - 1)
    near = lax.shift_right_logical(line, 2)
    reached = (near >= core) & (near < core + NEAR - 1) & (col < cols_dev + 2 * radius - 1)
    row = near * rows_dev + (row & (rows_dev - 1))
    active = reached & (base != 0.0) & (row > core * rows_dev)
    code[...] = ((row * 256 + col) * depth_bins + depth).astype(F32)
    places, counts = numbered(active.astype(F32))
    for j in range(blocks):
        place[:, j * LANES : (j + 1) * LANES] = places[j]
    total, most = jnp.int32(0), jnp.int32(0)
    n_units = NEAR * blocks
    for u in range(n_units):
        i = (u // blocks) * SLOTS + SLOTS - 1
        n = jnp.max(counts[u % blocks][i : i + 1, :]).astype(I32)
        units[0, u] = total
        units[1, u] = n
        total = total + n
        most = jnp.maximum(most, n)
    units[0, n_units] = total
    units[1, n_units] = most

    def write(u, first, size, row):
        codes[pl.ds(row, size), :] = gathered(place, code, u, blocks, first, size)

    in_windows(blocks, units.at[0], units.at[1], write)

    def ahead(g, carry):
        listed = live_rows(codes, pl.multiple_of(g * CHUNK, CHUNK), total)
        factors(
            listed, core, rows_dev, cols_dev, depth_bins, radius, planes.at[g], lines.at[g]
        )
        return carry

    lax.fori_loop(0, jnp.minimum(chunks_of(total), AHEAD), ahead, 0)


def profile(shifted, radius, wrapped=False):
    spread = SIGMA_SHARE * radius
    t = shifted.astype(F32) - radius
    within = shifted < 2 * radius
    if not wrapped:
        within = within & (shifted >= 0)
    return jnp.where(within, jnp.exp2(t * t * (-math.log2(math.e) / (2.0 * spread**2))), 0.0)


def factors(code, core, rows_dev, cols_dev, depth_bins, radius, planes, lines):
    depth = code[:, 0:1].astype(I32) & (depth_bins - 1)
    around = (iota((CHUNK, depth_bins), 1) + (radius - depth)) & (depth_bins - 1)
    lines[...] = profile(around, radius, wrapped=True)
    turned = jnp.concatenate(
        [code[i : i + LANES, :].T[0:1, :] for i in range(0, CHUNK, LANES)], axis=1
    ).astype(I32)
    shift = depth_bins.bit_length() - 1
    col = lax.shift_right_logical(turned, shift) & 255
    row = lax.shift_right_logical(turned, shift + 8)
    col_part = profile(iota((cols_dev, CHUNK), 0) - col + (2 * radius - 1), radius)
    for r in range(rows_dev):
        at = slice(r * cols_dev, (r + 1) * cols_dev)
        row_part = profile((core + CHIP) * rows_dev + r - row + radius, radius)
        hi, lo = parts_of(col_part * row_part, 2)
        planes[at, 0:CHUNK] = hi
        planes[at, CHUNK : 2 * CHUNK] = hi
        planes[at, 2 * CHUNK : 3 * CHUNK] = lo


def live_rows(array, start, total):
    live = iota((CHUNK, LANES), 0) + start < total
    return jnp.where(live, array[pl.ds(start, CHUNK), :], 0.0)


def chunks_of(total):
    return lax.div(total + (CHUNK - 1), CHUNK)


def deposit_kernel(
    rows_dev, cols_dev, radius,
    units, codes, place, planes, lines, quad, edge, bias, out, peak,
    heights, height, more_planes, more_lines, scaled,
):
    blocks = place.shape[1] // LANES
    depth_bins = bias.shape[1]
    core = lax.axis_index("c")
    lower = lax.axis_index("zl") == 0
    for k in range(CHIP):
        parts = edge[CHIP + k], quad[k], quad[CHIP + k], edge[k]
        for i in range(NEAR // CHIP):
            at = (i * CHIP + k) * SLOTS
            heights[at : at + SLOTS, :] = jnp.where(lower, parts[i], parts[i + 1])
    n_units = NEAR * blocks

    def write(u, first, size, row):
        height[pl.ds(row, size), :] = gathered(place, heights, u, blocks, first, size)

    in_windows(blocks, units.at[0], units.at[1], write)
    total = units[0, n_units]
    count = chunks_of(total)

    @pl.when(count == 0)
    def _():
        out[...] = bias[...]

    def add(g, plane, line, start=out):
        high = live_rows(height, pl.multiple_of(g * CHUNK, CHUNK), total)[:, 0:1]
        hi, lo = parts_of(line * high, 2)
        scaled[0:CHUNK, :] = hi
        scaled[CHUNK : 2 * CHUNK, :] = lo
        scaled[2 * CHUNK : 3 * CHUNK, :] = hi
        out[...] = start[...] + dot(plane, scaled[...])

    def ready(g, carry):
        add(g, planes[g], lines[g])
        return carry

    def rest(g, carry):
        code = live_rows(codes, pl.multiple_of(g * CHUNK, CHUNK), total)
        factors(code, core, rows_dev, cols_dev, depth_bins, radius, more_planes, more_lines)
        add(g, more_planes[...], more_lines[...])
        return carry

    @pl.when(count > 0)
    def _():
        add(0, planes[0], lines[0], bias)

    lax.fori_loop(1, jnp.minimum(count, AHEAD), ready, 0)
    lax.fori_loop(AHEAD, count, rest, 0)
    peak[...] = jnp.full(peak.shape, jnp.max(out[...]), F32)


def free_kernel(recv, bias, bias_out, out, free, sems):
    bias_copy = pltpu.make_async_copy(bias, bias_out, sems.at[STRIPS])
    bias_copy.start()
    highest = jnp.max(recv[...])
    size = bias.shape[0] // STRIPS
    copies = []
    for i in range(STRIPS):
        at = pl.ds(i * size, size)
        free[at, :] = FREE_SCALE * (highest - bias[at, :])
        copies.append(pltpu.make_async_copy(free.at[at, :], out.at[at, :], sems.at[i]))
        copies[-1].start()
    for c in copies:
        c.wait()
    bias_copy.wait()


def call(body, name, out_shape, *operands, smem=0, space=pltpu.VMEM, scratch=()):
    spaces = [pltpu.SMEM if i < smem else space for i in range(len(operands))]
    operands = [
        x if i < smem else pltpu.with_memory_space_constraint(x, space)
        for i, x in enumerate(operands)
    ]
    def space_of(shape):
        if isinstance(shape, jax.ShapeDtypeStruct):
            return pltpu.SMEM if shape.dtype == I32 else pltpu.HBM
        return pltpu.VMEM

    out_specs = jax.tree.map(lambda s: pl.BlockSpec(memory_space=space_of(s)), out_shape)
    return pl.pallas_call(
        body,
        name=name,
        out_shape=out_shape,
        in_specs=[pl.BlockSpec(memory_space=m) for m in spaces],
        out_specs=out_specs,
        scratch_shapes=list(scratch),
        compiler_params=pltpu.CompilerParams(vmem_limit_bytes=24 << 20),
    )(*operands)


def vmem(*dims):
    return pltpu.VMEM(dims, F32)


def hbm(*dims):
    return jax.ShapeDtypeStruct(dims, F32)


def swap(array, axes):
    return lax.all_to_all(array, axes, 0, 0, tiled=True)


def copied(array, axes):
    return swap(jnp.broadcast_to(array[None], (lax.axis_size(axes), *array.shape)), axes)


def per_device(
    bias_grid, hill_slab, hill_row, hill_col, hill_depth, hill_level, hill_count, height_levels
):
    rows_dev, cols_dev, depth_bins = bias_grid.shape
    n_slab = lax.axis_size(SLAB)
    n_walk = lax.axis_size("walk")
    radius = 2 * rows_dev
    grid_cols = cols_dev * n_walk
    senders = n_slab * n_walk
    cells = rows_dev * cols_dev
    chips = n_slab // CHIP
    blocks = senders // LANES
    rows = NEAR * SLOTS
    quads = 2 * CHIP

    message, bias = call(
        functools.partial(pack_kernel, rows_dev),
        "pack",
        (vmem(chips, LANES), vmem(cells, depth_bins)),
        hill_count,
        height_levels,
        hill_slab[:, :, 0],
        hill_row,
        hill_col,
        hill_depth,
        hill_level,
        bias_grid.reshape(cells, depth_bins),
        space=pltpu.HBM,
        scratch=[pltpu.SMEM(hill_count.shape, I32), pltpu.SMEM(height_levels.shape, F32)]
        + [pltpu.VMEM(hill_row.shape, I32)] * 5
        + [pltpu.SemaphoreType.DMA((8,))],
    )
    message = swap(message.reshape(chips, 1, LANES), ("y", "zh", "zl")).reshape(chips, LANES)
    recv = copied(message, CHIP_ROW).reshape(senders, LANES)

    own, table = call(
        functools.partial(height_kernel, cols_dev),
        "heights",
        (vmem(quads * n_walk, SLOTS, senders), vmem(LANES, senders)),
        recv,
        bias,
        scratch=[pltpu.VMEM((cells, depth_bins), BF16)] * 2
        + [pltpu.VMEM((CHIP * SLOTS, senders), F32)],
    )
    quad = swap(own, QUAD).reshape(quads, n_walk, SLOTS, senders).sum(axis=1)
    route = [(s, (s + (CHIP if s % quads >= CHIP else -CHIP)) % n_slab) for s in range(n_slab)]
    edge = lax.ppermute(quad, SLAB, route)

    most = (NEAR - 1) * SLOTS * senders + UNIT + SLOTS * LANES + LATER
    most = -(-most // CHUNK) * CHUNK
    codes, place, units, planes, lines = call(
        functools.partial(list_kernel, cols_dev, grid_cols, rows_dev, radius, depth_bins),
        "list",
        (
            vmem(most, LANES),
            vmem(rows, senders),
            jax.ShapeDtypeStruct((2, LANES), I32),
            pltpu.VMEM((AHEAD, cells, 3 * CHUNK), BF16),
            vmem(AHEAD, CHUNK, depth_bins),
        ),
        table,
        quad,
        scratch=[pltpu.VMEM((rows, senders), F32)],
    )
    near, far = ("zh", "zl", "c"), ("y", "walk")
    n_near, n_far = lax.axis_size(near), lax.axis_size(far)
    new_bias, peak = call(
        functools.partial(deposit_kernel, rows_dev, cols_dev, radius),
        "deposit",
        (vmem(cells, depth_bins), vmem(n_near, LANES)),
        units,
        codes,
        place,
        planes,
        lines,
        quad,
        edge,
        bias,
        smem=1,
        scratch=[
            pltpu.VMEM((rows, senders), F32),
            pltpu.VMEM((most, LANES), F32),
            pltpu.VMEM((cells, 3 * CHUNK), BF16),
            pltpu.VMEM((CHUNK, depth_bins), F32),
            pltpu.VMEM((3 * CHUNK, depth_bins), BF16),
        ],
    )
    peaks = swap(peak.reshape(n_near, 1, LANES), near).max(axis=0)
    peaks = swap(jnp.broadcast_to(peaks, (n_far, 1, LANES)), far).reshape(n_far, LANES)
    new_bias, free = call(
        free_kernel,
        "free",
        (hbm(cells, depth_bins), hbm(cells, depth_bins)),
        peaks,
        new_bias,
        scratch=[
            pltpu.VMEM((cells, depth_bins), F32),
            pltpu.SemaphoreType.DMA((STRIPS + 1,)),
        ],
    )
    return new_bias.reshape(bias_grid.shape), free.reshape(bias_grid.shape)


def solution(mesh):
    split = Mesh(mesh.devices.reshape(8, 4, 2, 2, mesh.shape["walk"]), EVERY)
    in_specs = (
        P(SLAB, "walk", None),
        P(EVERY, None, None),
        P(EVERY, None),
        P(EVERY, None),
        P(EVERY, None),
        P(EVERY, None),
        P(EVERY),
        P(),
    )
    out_specs = (P(SLAB, "walk", None), P(SLAB, "walk", None))
    return jax.shard_map(
        per_device, mesh=split, in_specs=in_specs, out_specs=out_specs, check_vma=False
    )
```
